32 devices in a mesh: dp: 4 (over y, x), tensor: 8 (over z, core).
Axes of the slice: x: 2, y: 2, z: 4, core: 2. Of those that a mesh axis runs over, the one named last changes fastest.
Arguments:
- queries: bfloat16 [1536, 8192], P('dp', 'tensor'), may hold values from -180 to 180
- keys: bfloat16 [1536, 1024], P('dp'), may hold values from -4.5 to 4.5
- values: bfloat16 [1536, 1024], P('dp'), may hold values from -6 to 6
- grad_out: bfloat16 [1536, 8192], P('dp', 'tensor'), may hold values from -3 to 3
- weight: float32 [8192, 8192], P('dp', 'tensor'), as said below
- first_code: bfloat16 [8192, 8192], P('dp', 'tensor'), may hold values from -1 to 1, as said below
- first_rows: float32 [8192], P('dp'), may hold values from 0.2 to 5
- first_cols: float32 [8192], P('tensor'), may hold values from 0.2 to 5
- second_code: bfloat16 [8192, 8192], P('dp', 'tensor'), may hold values from 0 to 1, as said below
- second_rows: float32 [8192], P('dp'), may hold values from 0.5 to 20
- second_cols: float32 [8192], P('tensor'), may hold values from 0.5 to 20
Outputs:
- grad_queries: bfloat16 [1536, 8192], P('dp', 'tensor')
- new_weight: float32 [8192, 8192], P('dp', 'tensor')
- next_first_code: bfloat16 [8192, 8192], P('dp', 'tensor')
- next_first_rows: float32 [8192], P('dp')
- next_first_cols: float32 [8192], P('tensor')
- next_second_code: bfloat16 [8192, 8192], P('dp', 'tensor')
- next_second_rows: float32 [8192], P('dp')
- next_second_cols: float32 [8192], P('tensor')
The draws below stay inside these ranges and needn't reach their ends.
Inputs may be any that keep to these rules, and one draw needn't show every extreme that they name: `weight`: rows 8192 onward are zero. `first_code`: rows 8192 onward are zero. `second_code`: rows 8192 onward are zero; all other entries are 0.05 or more.
All inputs are finite; a program needn't handle non-finite values.
Results may differ from the reference program's by a relative error of at most 0.023.
Values may be sent and summed in bfloat16 or wider, within the bound.
A program may use at most 128 MiB of HBM per device.

```python
import math
import jax
import jax.numpy as jnp
from jax import lax

D = 8192
H = 64
KVH = 8
HD = 128
SEQ = 384
TOK = 1536
CPAD = 8192


def paired_draw(key):
    count = TOK // SEQ
    queries = jnp.clip(jax.random.normal(jax.random.fold_in(key, 101), (count, SEQ, H * HD), jnp.float32), -4.5, 4.5)
    keys = jnp.clip(jax.random.normal(jax.random.fold_in(key, 102), (count, SEQ, KVH * HD), jnp.float32), -4.5, 4.5)
    return (queries.reshape(TOK, H * HD), keys.reshape(TOK, KVH * HD))


def draw_queries(key, part):
    return paired_draw(key)[0].astype(jnp.bfloat16)


def draw_keys(key, part):
    return paired_draw(key)[1].astype(jnp.bfloat16)


def real_rows():
    return jnp.arange(CPAD)[:, None] < D


def draw_weight(key, part):
    filled = jax.random.normal(key, (CPAD, H * HD), jnp.float32) * (H * HD) ** (-0.5)
    return jnp.where(real_rows(), filled, 0.0)


def draw_first_code(key, part):
    filled = jax.random.uniform(key, (CPAD, H * HD), jnp.float32, -1.0, 1.0)
    return jnp.where(real_rows(), filled, 0.0).astype(jnp.bfloat16)


def draw_second_code(key, part):
    filled = jax.random.uniform(key, (CPAD, H * HD), jnp.float32, 0.05, 1.0)
    return jnp.where(real_rows(), filled, 0.0).astype(jnp.bfloat16)


def levels(rng, dims, shards, smallest, largest):
    def one(position, parts):
        draws = jax.random.uniform(jax.random.fold_in(jax.random.fold_in(rng, 6), position), (parts,), jnp.float32, smallest / len(shards), largest / len(shards))
        return jnp.repeat(jnp.exp(draws), dims[position] // parts).reshape((-1,) + (1,) * (len(dims) - position - 1))

    loudness = one(*shards[0])
    for cut in shards[1:]:
        loudness = loudness * one(*cut)
    return loudness


def scatter_about(key, dims, spread, most, split=(), dtype=jnp.bfloat16):
    level = levels(key, dims, split, -0.22, 0.18) if split else 1.0
    array = jax.random.normal(key, dims, jnp.float32) * spread * level
    return jnp.minimum(jnp.maximum(array, -most), most).astype(dtype)


def setup_inputs(seed: int = 0) -> dict:
    streams_of = jax.random.split(jax.random.key(seed), 12)
    return {
        "queries": draw_queries(jax.random.fold_in(streams_of[11], 71), 0),
        "keys": draw_keys(jax.random.fold_in(streams_of[11], 71), 0),
        "values": scatter_about(streams_of[2], (TOK, KVH * HD), 1.0, 6.0, ((0, 4),)),
        "grad_out": scatter_about(streams_of[3], (TOK, D), 0.5, 3.0, ((0, 4), (1, 8))),
        "weight": draw_weight(jax.random.fold_in(streams_of[11], 71), 0),
        "first_code": draw_first_code(jax.random.fold_in(streams_of[11], 71), 0),
        "first_rows": jnp.clip(jnp.exp(math.log(5.0) - 3.218876 * jax.random.uniform(streams_of[6], (CPAD,), jnp.float32) ** levels(streams_of[6], (CPAD,), ((0, 4),), -0.2, 0.2)), 0.2, 5.0),
        "first_cols": jnp.clip(jnp.exp(math.log(5.0) - 3.218876 * jax.random.uniform(streams_of[7], (H * HD,), jnp.float32) ** levels(streams_of[7], (H * HD,), ((0, 8),), -0.2, 0.2)), 0.2, 5.0),
        "second_code": draw_second_code(jax.random.fold_in(streams_of[11], 71), 0),
        "second_rows": jnp.clip(jnp.exp(math.log(20.0) - 3.6888795 * jax.random.uniform(streams_of[9], (CPAD,), jnp.float32) ** levels(streams_of[9], (CPAD,), ((0, 4),), -0.2, 0.2)), 0.5, 20.0),
        "second_cols": jnp.clip(jnp.exp(math.log(20.0) - 3.6888795 * jax.random.uniform(streams_of[10], (H * HD,), jnp.float32) ** levels(streams_of[10], (H * HD,), ((0, 8),), -0.2, 0.2)), 0.5, 20.0),
    }


beta_first = 0.9
beta_second = 0.95
learning = 0.01
decay_rate = 0.1
adam_eps = 1e-08
code_eps = 1e-06
correct_first = 1.0 - 0.9 ** 10
correct_second = 1.0 - 0.95 ** 10

def reference(queries, keys, values, grad_out, weight, first_code, first_rows, first_cols, second_code, second_rows, second_cols):
    count = queries.shape[0] // SEQ
    group = H // KVH
    factor = HD ** (-0.5)
    weight_half = weight.astype(jnp.bfloat16)
    grad_att = jnp.dot(grad_out, weight_half[:D], preferred_element_type=jnp.float32)
    grad_half = grad_att.astype(jnp.bfloat16)
    future = jnp.arange(SEQ)[None, :] > jnp.arange(SEQ)[:, None]

    def per_sequence(inputs):
        query_block, key_block, value_block, grad_block = inputs
        query_heads = query_block.reshape(SEQ, H, HD).astype(jnp.float32)
        key_heads = jnp.repeat(key_block.reshape(SEQ, KVH, HD), group, axis=1).astype(jnp.float32)
        value_heads = jnp.repeat(value_block.reshape(SEQ, KVH, HD), group, axis=1).astype(jnp.float32)
        scores = jnp.einsum('qhd,khd->hqk', query_heads, key_heads) * factor
        scores = jnp.where(future[None], -1e+30, scores)
        highest = lax.optimization_barrier(jnp.max(scores, axis=-1, keepdims=True))
        exponent = jnp.exp(scores - highest)
        probabilities = exponent / lax.optimization_barrier(jnp.sum(exponent, axis=-1, keepdims=True))
        weights_half = probabilities.astype(jnp.bfloat16)
        attended = jnp.einsum('hqk,khd->qhd', weights_half.astype(jnp.float32), value_heads).astype(jnp.bfloat16)
        grad_heads = grad_block.reshape(SEQ, H, HD).astype(jnp.float32)
        grad_probs = jnp.einsum('qhd,khd->hqk', grad_heads, value_heads)
        row_dot = lax.optimization_barrier(jnp.sum(grad_heads * attended.astype(jnp.float32), axis=-1))
        grad_scores = (probabilities * (grad_probs - row_dot.T[:, :, None])).astype(jnp.bfloat16)
        grad_query = (jnp.einsum('hqk,khd->qhd', grad_scores.astype(jnp.float32), key_heads) * factor).astype(jnp.bfloat16)
        return (grad_query.reshape(SEQ, H * HD), attended.reshape(SEQ, H * HD))
    grad_queries, attended = lax.map(per_sequence, (queries.reshape(count, SEQ, H * HD), keys.reshape(count, SEQ, KVH * HD), values.reshape(count, SEQ, KVH * HD), grad_half.reshape(count, SEQ, H * HD)))

    def accumulate(total, inputs):
        grad_block, att_block = inputs
        term = jnp.dot(grad_block.T, att_block, preferred_element_type=jnp.float32)
        return (total + lax.optimization_barrier(term.astype(jnp.bfloat16)).astype(jnp.float32), 0)
    weight_grad, unused = lax.scan(accumulate, jnp.zeros((D, H * HD), jnp.float32), (grad_out.reshape(count, SEQ, D), attended))
    weight_grad = jnp.pad(weight_grad, ((0, CPAD - D), (0, 0)))
    first = first_code.astype(jnp.float32) * jnp.minimum(first_rows[:, None], first_cols[None, :])
    second = second_code.astype(jnp.float32) * jnp.minimum(second_rows[:, None], second_cols[None, :])
    first_new = beta_first * first + (1.0 - beta_first) * weight_grad
    second_new = beta_second * second + (1.0 - beta_second) * weight_grad * weight_grad
    step_size = first_new / correct_first / (jnp.sqrt(second_new / correct_second) + adam_eps)
    new_weight = weight - learning * (step_size + decay_rate * weight)
    first_abs = jnp.abs(first_new)
    second_abs = jnp.abs(second_new)
    next_first_rows = lax.optimization_barrier(jnp.max(first_abs, axis=1))
    next_first_cols = lax.optimization_barrier(jnp.max(first_abs, axis=0))
    next_second_rows = lax.optimization_barrier(jnp.max(second_abs, axis=1))
    next_second_cols = lax.optimization_barrier(jnp.max(second_abs, axis=0))
    next_first_code = (first_new / (jnp.minimum(next_first_rows[:, None], next_first_cols[None, :]) + code_eps)).astype(jnp.bfloat16)
    next_second_code = (second_new / (jnp.minimum(next_second_rows[:, None], next_second_cols[None, :]) + code_eps)).astype(jnp.bfloat16)
    return (grad_queries.reshape(count * SEQ, H * HD), new_weight, next_first_code, next_first_rows, next_first_cols, next_second_code, next_second_rows, next_second_cols)
```

```python
import jax
import jax.numpy as jnp
from jax import lax
from jax.sharding import PartitionSpec as P

H = 64
KVH = 8
HD = 128


beta_first = 0.9
beta_second = 0.95
learning = 0.01
decay_rate = 0.1
adam_eps = 1e-08
code_eps = 1e-06
correct_first = 1.0 - 0.9**10
correct_second = 1.0 - 0.95**10


def attend(queries, key_sel, value_sel, heads_dev):
    length = queries.shape[0]
    query_heads = queries.reshape(length, heads_dev, HD)
    scores = jnp.einsum(
        "qhd,kd->hqk", query_heads, key_sel, preferred_element_type=jnp.float32
    ) * HD ** (-0.5)
    future = lax.broadcasted_iota(jnp.int32, (length, length), 1) > lax.broadcasted_iota(
        jnp.int32, (length, length), 0
    )
    scores = jnp.where(future[None], -1e30, scores)
    highest = jnp.max(scores, axis=-1, keepdims=True)
    exponent = jnp.exp(scores - highest)
    probabilities = exponent / jnp.sum(exponent, axis=-1, keepdims=True)
    weights_half = probabilities.astype(jnp.bfloat16)
    attended = jnp.einsum(
        "hqk,kd->qhd", weights_half, value_sel, preferred_element_type=jnp.float32
    )
    return (probabilities, attended.astype(jnp.bfloat16).reshape(length, heads_dev * HD))


def attend_back(probabilities, attended, grad_half, key_sel, value_sel, heads_dev):
    length = grad_half.shape[0]
    grad_heads = grad_half.reshape(length, heads_dev, HD)
    grad_probs = jnp.einsum(
        "qhd,kd->hqk", grad_heads, value_sel, preferred_element_type=jnp.float32
    )
    row_dot = jnp.sum(
        grad_heads.astype(jnp.float32)
        * attended.reshape(length, heads_dev, HD).astype(jnp.float32),
        axis=-1,
    )
    grad_scores = (probabilities * (grad_probs - row_dot.T[:, :, None])).astype(jnp.bfloat16)
    grad_query = jnp.einsum(
        "hqk,kd->qhd", grad_scores, key_sel, preferred_element_type=jnp.float32
    ) * HD ** (-0.5)
    return grad_query.astype(jnp.bfloat16).reshape(length, heads_dev * HD)


def per_device(
    queries,
    keys,
    values,
    grad_out,
    weight,
    first_code,
    first_rows,
    first_cols,
    second_code,
    second_rows,
    second_cols,
):
    dp_count = lax.axis_size("dp")
    cols_dev = queries.shape[1]
    heads_dev = cols_dev // HD
    rows_dev = weight.shape[0]
    width_pad = dp_count * rows_dev
    tensor_index = lax.axis_index("tensor")
    kv_start = tensor_index * heads_dev // (H // KVH) * HD
    weight_half = weight.astype(jnp.bfloat16)
    length = queries.shape[0]
    gathered = lax.all_gather(grad_out, "tensor", axis=0)
    tensor_count, unused, feats = gathered.shape
    if rows_dev % feats == 0 and width_pad == tensor_count * feats:
        pieces = rows_dev // feats
        blocks = gathered.reshape(dp_count, pieces, length, feats)
    else:
        pieces = 1
        flat = jnp.moveaxis(gathered, 0, 1).reshape(length, tensor_count * feats)
        flat = jnp.pad(flat, ((0, 0), (0, width_pad - flat.shape[1])))
        blocks = jnp.moveaxis(flat.reshape(length, dp_count, 1, rows_dev), 0, 2)
    key_sel = lax.dynamic_slice_in_dim(keys, kv_start, HD, 1)
    value_sel = lax.dynamic_slice_in_dim(values, kv_start, HD, 1)
    probabilities, attended = attend(queries, key_sel, value_sel, heads_dev)
    all_attended = lax.all_gather(attended, "dp", axis=0, tiled=True)
    mine = lax.all_to_all(blocks, "dp", 0, 0, tiled=True)
    span = rows_dev // pieces
    parts = [mine[:, k].reshape(dp_count * length, span) for k in range(pieces)]
    partial = sum(
        jnp.dot(
            parts[k], weight_half[k * span : (k + 1) * span], preferred_element_type=jnp.float32
        )
        for k in range(pieces)
    )
    grad_half = lax.psum_scatter(
        partial.astype(jnp.bfloat16), "dp", scatter_dimension=0, tiled=True
    )
    weight_grad = jnp.concatenate(
        [
            jnp.einsum("sc,sh->ch", parts[k], all_attended, preferred_element_type=jnp.float32)
            for k in range(pieces)
        ],
        axis=0,
    )
    grad_queries = attend_back(probabilities, attended, grad_half, key_sel, value_sel, heads_dev)
    first = first_code.astype(jnp.float32) * jnp.minimum(first_rows[:, None], first_cols[None, :])
    second = second_code.astype(jnp.float32) * jnp.minimum(
        second_rows[:, None], second_cols[None, :]
    )
    first_new = beta_first * first + (1.0 - beta_first) * weight_grad
    second_new = beta_second * second + (1.0 - beta_second) * weight_grad * weight_grad
    step_size = first_new / correct_first / (jnp.sqrt(second_new / correct_second) + adam_eps)
    new_weight = weight - learning * (step_size + decay_rate * weight)
    first_abs = jnp.abs(first_new)
    second_abs = jnp.abs(second_new)
    local_rows_max = jnp.stack([jnp.max(first_abs, axis=1), jnp.max(second_abs, axis=1)])
    local_cols_max = jnp.stack([jnp.max(first_abs, axis=0), jnp.max(second_abs, axis=0)])
    rows_mine = lax.pmax(local_rows_max, "tensor")
    cols_mine = lax.pmax(local_cols_max, "dp")
    next_first_code = (
        first_new / (jnp.minimum(rows_mine[0][:, None], cols_mine[0][None, :]) + code_eps)
    ).astype(jnp.bfloat16)
    next_second_code = (
        second_new / (jnp.minimum(rows_mine[1][:, None], cols_mine[1][None, :]) + code_eps)
    ).astype(jnp.bfloat16)
    return (
        grad_queries,
        new_weight,
        next_first_code,
        rows_mine[0],
        cols_mine[0],
        next_second_code,
        rows_mine[1],
        cols_mine[1],
    )


def solution(mesh):
    return jax.shard_map(
        per_device,
        mesh=mesh,
        in_specs=(
            P("dp", "tensor"),
            P("dp", None),
            P("dp", None),
            P("dp", "tensor"),
            P("dp", "tensor"),
            P("dp", "tensor"),
            P("dp"),
            P("tensor"),
            P("dp", "tensor"),
            P("dp"),
            P("tensor"),
        ),
        out_specs=(
            P("dp", "tensor"),
            P("dp", "tensor"),
            P("dp", "tensor"),
            P("dp"),
            P("tensor"),
            P("dp", "tensor"),
            P("dp"),
            P("tensor"),
        ),
        check_vma=False,
    )
```

```python
import functools

import jax
import jax.numpy as jnp
from jax import lax
from jax.experimental import pallas as pl
from jax.experimental.pallas import tpu as pltpu
from jax.sharding import PartitionSpec as P

H = 64
KVH = 8
HD = 128


beta_first = 0.9
beta_second = 0.95
learning = 0.01
decay_rate = 0.1
adam_eps = 1e-08
code_eps = 1e-06
correct_first = 1.0 - 0.9**10
correct_second = 1.0 - 0.95**10


def attend(queries, key_sel, value_sel, heads_dev):
    length = queries.shape[0]
    query_heads = queries.reshape(length, heads_dev, HD)
    scores = jnp.einsum(
        "qhd,kd->hqk", query_heads, key_sel, preferred_element_type=jnp.float32
    ) * HD ** (-0.5)
    future = lax.broadcasted_iota(jnp.int32, (length, length), 1) > lax.broadcasted_iota(
        jnp.int32, (length, length), 0
    )
    scores = jnp.where(future[None], -1e30, scores)
    highest = jnp.max(scores, axis=-1, keepdims=True)
    exponent = jnp.exp(scores - highest)
    probabilities = exponent / jnp.sum(exponent, axis=-1, keepdims=True)
    weights_half = probabilities.astype(jnp.bfloat16)
    attended = jnp.einsum(
        "hqk,kd->qhd", weights_half, value_sel, preferred_element_type=jnp.float32
    )
    return (probabilities, attended.astype(jnp.bfloat16).reshape(length, heads_dev * HD))


def attend_back(probabilities, attended, grad_half, key_sel, value_sel, heads_dev):
    length = grad_half.shape[0]
    grad_heads = grad_half.reshape(length, heads_dev, HD)
    grad_probs = jnp.einsum(
        "qhd,kd->hqk", grad_heads, value_sel, preferred_element_type=jnp.float32
    )
    row_dot = jnp.sum(
        grad_heads.astype(jnp.float32)
        * attended.reshape(length, heads_dev, HD).astype(jnp.float32),
        axis=-1,
    )
    grad_scores = (probabilities * (grad_probs - row_dot.T[:, :, None])).astype(jnp.bfloat16)
    grad_query = jnp.einsum(
        "hqk,kd->qhd", grad_scores, key_sel, preferred_element_type=jnp.float32
    ) * HD ** (-0.5)
    return grad_query.astype(jnp.bfloat16).reshape(length, heads_dev * HD)


CORES = 2
CHUNKS = 2


def exchange_kernel(
    nd, nz, grad_ref, att_ref, g_ref, a_ref, zbuf,
    up_send, down_send, z_recv, own_send, d_send, d_recv, p_send, p_recv, a_send, a_recv, local_sem,
):
    d = lax.axis_index("dp")
    t = lax.axis_index("tensor")
    z = t // CORES
    c = t % CORES
    partner = t + 1 - 2 * c
    rows = grad_ref.shape[0] // CHUNKS
    has_up = z < nz - 1
    has_down = z > 0
    barrier = pltpu.get_barrier_semaphore()

    def greet(**where):
        pl.semaphore_signal(barrier, inc=1, device_id=where)

    greet(tensor=partner)
    for o in range(1, nd):
        greet(dp=(d + o) % nd)

    for o in range(1, nz):
        greet(tensor=(t + CORES * o) % (CORES * nz))
    pl.semaphore_wait(barrier, nd + nz - 1)

    def part(ch):
        return pl.ds(ch * rows, rows)

    def block(zp, ch, own):
        return grad_ref.at[part(ch)] if own else zbuf.at[zp, part(ch)]

    def up(zp, ch, own):
        return pltpu.make_async_remote_copy(
            block(zp, ch, own), zbuf.at[zp, part(ch)], up_send.at[zp, ch], z_recv.at[zp, ch],
            device_id={"tensor": t + CORES},
        )

    def down(zp, ch, own):
        return pltpu.make_async_remote_copy(
            block(zp, ch, own), zbuf.at[zp, part(ch)], down_send.at[zp, ch], z_recv.at[zp, ch],
            device_id={"tensor": t - CORES},
        )

    def to_owner(zp, ch, own):
        return pltpu.make_async_remote_copy(
            block(zp, ch, own), g_ref.at[d, c, part(ch)], d_send.at[zp, ch], d_recv.at[d, ch],
            device_id={"dp": zp},
        )

    def keep(zp, ch, own):
        return pltpu.make_async_copy(
            block(zp, ch, own), g_ref.at[d, c, part(ch)], local_sem.at[ch]
        )

    def keep_partner(zp, ch, own):
        return pltpu.make_async_remote_copy(
            block(zp, ch, own), g_ref.at[d, c, part(ch)], own_send.at[ch], p_recv.at[d, ch],
            device_id={"tensor": partner},
        )

    def to_partner(dp, ch):
        return pltpu.make_async_remote_copy(
            g_ref.at[dp, c, part(ch)], g_ref.at[dp, c, part(ch)], p_send.at[dp, ch],
            p_recv.at[dp, ch], device_id={"tensor": partner},
        )

    def att_copy(o):
        return pltpu.make_async_remote_copy(
            att_ref, a_ref.at[d], a_send.at[o], a_recv.at[o], device_id={"dp": (d + o) % nd}
        )

    def spread(zp, ch, own, act):
        @pl.when(zp == d)
        def _():
            act(keep_partner(zp, ch, own), True)
            act(keep(zp, ch, own), False)

        @pl.when(zp != d)
        def _():
            act(to_owner(zp, ch, own), True)

    def start(copy, remote):
        copy.start()

    def finish(copy, remote):
        if remote:
            copy.wait_send()
        else:
            copy.wait()

    for ch in range(CHUNKS):

        @pl.when(has_up)
        def _():
            up(z, ch, True).start()

        @pl.when(has_down)
        def _():
            down(z, ch, True).start()

        spread(z, ch, True, start)
    for o in range(1, nd):
        att_copy(o).start()
    own_att = pltpu.make_async_copy(att_ref, a_ref.at[d], local_sem.at[CHUNKS])
    own_att.start()

    for dist in range(1, nz):
        for ch in range(CHUNKS):

            @pl.when(z - dist >= 0)
            def _():
                zp = z - dist
                down(zp, ch, False).wait_recv()

                @pl.when(has_up)
                def _():
                    up(zp, ch, False).start()

                spread(zp, ch, False, start)

            @pl.when(z + dist < nz)
            def _():
                zp = z + dist
                down(zp, ch, False).wait_recv()

                @pl.when(has_down)
                def _():
                    down(zp, ch, False).start()

                spread(zp, ch, False, start)

    for ch in range(CHUNKS):
        for o in range(1, nd):
            src = (d + o) % nd
            pltpu.make_async_remote_copy(
                g_ref.at[src, c, part(ch)], g_ref.at[src, c, part(ch)], p_send.at[src, ch],
                d_recv.at[src, ch], device_id={"tensor": partner},
            ).wait_recv()
            to_partner(src, ch).start()

    own_att.wait()
    for o in range(1, nd):
        att_copy(o).wait_send()
        pltpu.make_async_remote_copy(
            att_ref, a_ref.at[(d + nd - o) % nd], a_send.at[o], a_recv.at[o],
            device_id={"dp": (d + o) % nd},
        ).wait_recv()
    for ch in range(CHUNKS):
        for src in range(nd):
            pltpu.make_async_remote_copy(
                g_ref.at[src, 1 - c, part(ch)], g_ref.at[src, 1 - c, part(ch)],
                p_send.at[src, ch], p_recv.at[src, ch], device_id={"tensor": partner},
            ).wait_recv()
        for o in range(1, nd):
            to_partner((d + o) % nd, ch).wait_send()

        @pl.when(has_up)
        def _():
            up(z, ch, True).wait_send()

        @pl.when(has_down)
        def _():
            down(z, ch, True).wait_send()

        spread(z, ch, True, finish)
        for dist in range(1, nz):

            @pl.when(z - dist >= 0)
            def _():
                @pl.when(has_up)
                def _():
                    up(z - dist, ch, False).wait_send()

                spread(z - dist, ch, False, finish)

            @pl.when(z + dist < nz)
            def _():
                @pl.when(has_down)
                def _():
                    down(z + dist, ch, False).wait_send()

                spread(z + dist, ch, False, finish)


def exchange(grad_out, attended, nd, nz):
    length, feats = grad_out.shape
    dma = pltpu.SemaphoreType.DMA
    return pl.pallas_call(
        functools.partial(exchange_kernel, nd, nz),
        out_shape=(
            jax.ShapeDtypeStruct((nd, CORES, length, feats), grad_out.dtype),
            jax.ShapeDtypeStruct((nd,) + attended.shape, attended.dtype),
        ),
        in_specs=[pl.BlockSpec(memory_space=pltpu.VMEM)] * 2,
        out_specs=(pl.BlockSpec(memory_space=pl.ANY),) * 2,
        scratch_shapes=[
            pltpu.VMEM((nz, length, feats), grad_out.dtype),
            dma((nz, CHUNKS)),
            dma((nz, CHUNKS)),
            dma((nz, CHUNKS)),
            dma((CHUNKS,)),
            dma((nz, CHUNKS)),
            dma((nd, CHUNKS)),
            dma((nd, CHUNKS)),
            dma((nd, CHUNKS)),
            dma((nd,)),
            dma((nd,)),
            dma((CHUNKS + 1,)),
        ],
        compiler_params=pltpu.CompilerParams(collective_id=0, has_side_effects=True),
    )(grad_out, attended)


def maxima_kernel(nd, nt, r_ref, c_ref, ro_ref, co_ref, rbuf, cbuf, rs, rr, cs, cr):
    d = lax.axis_index("dp")
    t = lax.axis_index("tensor")
    barrier = pltpu.get_barrier_semaphore()
    for o in range(1, nt):
        pl.semaphore_signal(barrier, inc=1, device_id={"tensor": (t + o) % nt})
    for o in range(1, nd):
        pl.semaphore_signal(barrier, inc=1, device_id={"dp": (d + o) % nd})
    pl.semaphore_wait(barrier, nt + nd - 2)
    copies = [
        pltpu.make_async_remote_copy(
            r_ref, rbuf.at[o], rs.at[o], rr.at[o], device_id={"tensor": (t + o) % nt}
        )
        for o in range(1, nt)
    ] + [
        pltpu.make_async_remote_copy(
            c_ref, cbuf.at[o], cs.at[o], cr.at[o], device_id={"dp": (d + o) % nd}
        )
        for o in range(1, nd)
    ]
    for copy in copies:
        copy.start()
    for copy in copies:
        copy.wait()
    rows = r_ref[...]
    for o in range(1, nt):
        rows = jnp.maximum(rows, rbuf[o])
    ro_ref[...] = rows
    cols = c_ref[...]
    for o in range(1, nd):
        cols = jnp.maximum(cols, cbuf[o])
    co_ref[...] = cols


def maxima(rows, cols, nd, nt):
    dma = pltpu.SemaphoreType.DMA
    vmem = pl.BlockSpec(memory_space=pltpu.VMEM)
    return pl.pallas_call(
        functools.partial(maxima_kernel, nd, nt),
        out_shape=(
            jax.ShapeDtypeStruct(rows.shape, rows.dtype),
            jax.ShapeDtypeStruct(cols.shape, cols.dtype),
        ),
        in_specs=[vmem] * 2,
        out_specs=(vmem,) * 2,
        scratch_shapes=[
            pltpu.VMEM((nt,) + rows.shape, rows.dtype),
            pltpu.VMEM((nd,) + cols.shape, cols.dtype),
            dma((nt,)),
            dma((nt,)),
            dma((nd,)),
            dma((nd,)),
        ],
        compiler_params=pltpu.CompilerParams(collective_id=1, has_side_effects=True),
    )(rows, cols)


def per_device(
    queries,
    keys,
    values,
    grad_out,
    weight,
    first_code,
    first_rows,
    first_cols,
    second_code,
    second_rows,
    second_cols,
):
    dp_count = lax.axis_size("dp")
    cols_dev = queries.shape[1]
    heads_dev = cols_dev // HD
    rows_dev = weight.shape[0]
    width_pad = dp_count * rows_dev
    tensor_index = lax.axis_index("tensor")
    kv_start = tensor_index * heads_dev // (H // KVH) * HD
    weight_half = weight.astype(jnp.bfloat16)
    length = queries.shape[0]
    key_sel = lax.dynamic_slice_in_dim(keys, kv_start, HD, 1)
    value_sel = lax.dynamic_slice_in_dim(values, kv_start, HD, 1)
    probabilities, attended = attend(queries, key_sel, value_sel, heads_dev)
    tensor_count, feats = lax.axis_size("tensor"), grad_out.shape[1]
    if rows_dev == CORES * feats and tensor_count == CORES * dp_count and length % 32 == 0:
        pieces = CORES
        mine, all_attended = exchange(grad_out, attended, dp_count, tensor_count // CORES)
        all_attended = all_attended.reshape(dp_count * length, cols_dev)
    else:
        pieces = 1
        flat = lax.all_gather(grad_out, "tensor", axis=1, tiled=True)
        flat = jnp.pad(flat, ((0, 0), (0, width_pad - flat.shape[1])))
        blocks = jnp.moveaxis(flat.reshape(length, dp_count, 1, rows_dev), 0, 2)
        mine = lax.all_to_all(blocks, "dp", 0, 0, tiled=True)
        all_attended = lax.all_gather(attended, "dp", axis=0, tiled=True)
    span = rows_dev // pieces
    parts = [mine[:, k].reshape(dp_count * length, span) for k in range(pieces)]
    partial = sum(
        jnp.dot(
            parts[k], weight_half[k * span : (k + 1) * span], preferred_element_type=jnp.float32
        )
        for k in range(pieces)
    )
    partial, all_attended = lax.optimization_barrier(
        (partial.astype(jnp.bfloat16), all_attended)
    )
    grad_half = lax.psum_scatter(
        partial, "dp", scatter_dimension=0, tiled=True
    )
    weight_grad = jnp.concatenate(
        [
            jnp.einsum("sc,sh->ch", parts[k], all_attended, preferred_element_type=jnp.float32)
            for k in range(pieces)
        ],
        axis=0,
    )
    grad_queries = attend_back(probabilities, attended, grad_half, key_sel, value_sel, heads_dev)
    first = first_code.astype(jnp.float32) * jnp.minimum(first_rows[:, None], first_cols[None, :])
    second = second_code.astype(jnp.float32) * jnp.minimum(
        second_rows[:, None], second_cols[None, :]
    )
    first_new = beta_first * first + (1.0 - beta_first) * weight_grad
    second_new = beta_second * second + (1.0 - beta_second) * weight_grad * weight_grad
    step_size = first_new / correct_first / (jnp.sqrt(second_new / correct_second) + adam_eps)
    new_weight = weight - learning * (step_size + decay_rate * weight)
    first_abs = jnp.abs(first_new)
    second_abs = jnp.abs(second_new)
    local_rows_max = jnp.stack([jnp.max(first_abs, axis=1), jnp.max(second_abs, axis=1)])
    local_cols_max = jnp.stack([jnp.max(first_abs, axis=0), jnp.max(second_abs, axis=0)])
    rows_mine, cols_mine = maxima(local_rows_max, local_cols_max, dp_count, tensor_count)
    next_first_code = (
        first_new / (jnp.minimum(rows_mine[0][:, None], cols_mine[0][None, :]) + code_eps)
    ).astype(jnp.bfloat16)
    next_second_code = (
        second_new / (jnp.minimum(rows_mine[1][:, None], cols_mine[1][None, :]) + code_eps)
    ).astype(jnp.bfloat16)
    return (
        grad_queries,
        new_weight,
        next_first_code,
        rows_mine[0],
        cols_mine[0],
        next_second_code,
        rows_mine[1],
        cols_mine[1],
    )


def solution(mesh):
    return jax.shard_map(
        per_device,
        mesh=mesh,
        in_specs=(
            P("dp", "tensor"),
            P("dp", None),
            P("dp", None),
            P("dp", "tensor"),
            P("dp", "tensor"),
            P("dp", "tensor"),
            P("dp"),
            P("tensor"),
            P("dp", "tensor"),
            P("dp"),
            P("tensor"),
        ),
        out_specs=(
            P("dp", "tensor"),
            P("dp", "tensor"),
            P("dp", "tensor"),
            P("dp"),
            P("tensor"),
            P("dp", "tensor"),
            P("dp"),
            P("tensor"),
        ),
        check_vma=False,
    )
```
